512 devices in a mesh: row: 8 (over z_hi, core), col: 16 (over y, z_lo), dp: 4 (over x).
Axes of the slice: x: 4, y: 4, z: 16 (z_hi: 4, z_lo: 4; z = z_hi * 4 + z_lo), core: 2. Of those that a mesh axis runs over, the one named last changes fastest.
Arguments:
- activations: bfloat16 [4, 1024, 16384], P('dp', 'col', 'row'), may hold values from -6 to 6
- out_grads: bfloat16 [4, 1024, 4096], P('dp', 'row', 'col'), may hold values from -6 to 6
- block_mask: int32 [128, 32], P('row', 'col'), may hold values from 0 to 1, as said below
- master_weight: float32 [16384, 4096], P(('row', 'dp'), 'col'), may hold values from -0.046875 to 0.046875
- first_moment: float32 [16384, 4096], P(('row', 'dp'), 'col'), may hold values from -12 to 12
- second_moment: float32 [16384, 4096], P(('row', 'dp'), 'col'), may hold values from 0.05 to 2
Outputs:
- input_grads: bfloat16 [4, 1024, 16384], P('dp', 'col', 'row')
- new_weight: float32 [16384, 4096], P(('row', 'dp'), 'col')
- new_first: float32 [16384, 4096], P(('row', 'dp'), 'col')
- new_second: float32 [16384, 4096], P(('row', 'dp'), 'col')
The draws below stay inside these ranges and needn't reach their ends.
Inputs may be any that keep to these rules, and one draw needn't show every extreme that they name: `block_mask`: 1 where the 128 x 128 block of the weight is kept, 0 where it is pruned.
All inputs are finite; a program needn't handle non-finite values.
Results may differ from the reference program's by a relative error of at most 0.015.
Values may be sent and summed in bfloat16 or wider, within the bound.
No kernel may reach another device: no remote copies, remote signals or barrier semaphores. Data moves between devices by JAX's collectives and lax.ppermute only.
A program may use at most 64 MiB of HBM per device.

```python
import math
import jax
import jax.numpy as jnp
from jax import lax

D = 4096
FF = 16384
BLOCK = 128
TOK_G = 1024
GROUPS = 4
N_COL = 16


def draw_block_mask(key, part):
    band_key = jax.random.fold_in(key, 11)
    cell_key = jax.random.fold_in(key, 12)
    levels = jax.random.randint(band_key, (FF // BLOCK // 4, 1), 15, 86)
    levels = jnp.repeat(levels, 4, axis=0)
    scores = jax.random.randint(cell_key, (FF // BLOCK, D // BLOCK), 0, 100)
    return (scores < levels).astype(jnp.int32)


def with_spikes(result, own_key, source, target, shards_of, factor):
    def block_of(position):
        return (jnp.arange(result.shape[position]) // (result.shape[position] // shards_of)).reshape((-1,) + (1,) * (result.ndim - 1 - position))

    first = jax.random.permutation(own_key, shards_of)[block_of(target)]
    second = (block_of(target) + shards_of // 2) % shards_of
    return jnp.where((block_of(source) == first) | (block_of(source) == second), factor * result, result)


def shard_levels(stream_key, shape, pieces, low, top_value):
    factor_of, own = 1.0, jax.random.fold_in(stream_key, 6)
    for position, blocks in pieces:
        steps = jnp.exp(jax.random.uniform(jax.random.fold_in(own, position), (blocks,), jnp.float32, low / len(pieces), top_value / len(pieces)))
        factor_of = factor_of * jnp.repeat(steps, shape[position] // blocks).reshape([-1 if axis == position else 1 for axis in range(len(shape))])
    return factor_of


def bell_draw(key, shape, width, reach, shards=(), held_as=jnp.bfloat16):
    loudness = shard_levels(key, shape, shards, -0.22, 0.18) if shards else 1.0
    drawn = jax.random.normal(key, shape, jnp.float32) * width * loudness
    return jnp.minimum(jnp.maximum(drawn, -reach), reach).astype(held_as)


def gaussian_with(rng, shape, width, bound, cuts, heavy, kind=jnp.bfloat16):
    drawn = width * jax.random.normal(rng, shape, jnp.float32)
    if cuts:
        drawn = drawn * shard_levels(rng, shape, cuts, -0.22, 0.18)
    return jnp.clip(with_spikes(drawn, jax.random.fold_in(rng, 3), *heavy), -bound, bound).astype(kind)


def setup_inputs(seed: int = 0) -> dict:
    seeds = jax.random.split(jax.random.key(seed), 7)
    activations = bell_draw(seeds[0], (GROUPS, TOK_G, FF), 1.0, 6.0, ((0, 4), (1, 16), (2, 8)))
    out_grads = gaussian_with(seeds[1], (GROUPS, TOK_G, D), 1.0, 6.0, ((0, 4), (1, 8), (2, 16)), (2, 1, 16, 2.0))
    block_mask = draw_block_mask(jax.random.fold_in(seeds[6], 71), 0)
    master_weight = bell_draw(seeds[3], (FF, D), FF ** -0.5, 0.046875, ((0, 32), (1, 16)), jnp.float32)
    first_moment = bell_draw(seeds[4], (FF, D), 2.0, 12.0, ((0, 32), (1, 16)), jnp.float32)
    second_moment = jnp.clip(jnp.exp(math.log(2.0) - 3.6888794 * jax.random.uniform(seeds[5], (FF, D), jnp.float32) ** shard_levels(seeds[5], (FF, D), ((0, 32), (1, 16)), -0.2, 0.2)), 0.05, 2.0)
    return dict(activations=activations, out_grads=out_grads, block_mask=block_mask, master_weight=master_weight, first_moment=first_moment, second_moment=second_moment)


first_decay = 0.9
second_decay = 0.999
learn_rate = 0.001
adam_epsilon = 1e-08
first_correct = 1.0 - 0.9 ** 10
second_correct = 1.0 - 0.999 ** 10

def expand(block_keep):
    tall, broad = block_keep.shape
    values = block_keep.astype(jnp.float32)
    grown = jnp.broadcast_to(values[:, None, :, None], (tall, BLOCK, broad, BLOCK))
    return grown.reshape(tall * BLOCK, broad * BLOCK)

def reference(activations, out_grads, block_mask, master_weight, first_moment, second_moment):
    keep = expand(block_mask)
    pruned = master_weight.astype(jnp.bfloat16) * keep.astype(jnp.bfloat16)
    col_width = D // N_COL

    def group_inputs(grad_group):

        def add_column(index, running):
            offset = (index * col_width).astype(jnp.int32)
            grad_cols = lax.dynamic_slice_in_dim(grad_group, offset, col_width, 1)
            weight_cols = lax.dynamic_slice_in_dim(pruned, offset, col_width, 1)
            partial_value = jnp.dot(grad_cols, weight_cols.T, preferred_element_type=jnp.float32)
            rounded = lax.optimization_barrier(partial_value.astype(jnp.bfloat16))
            return running + rounded.astype(jnp.float32)
        start_sum = jnp.zeros((grad_group.shape[0], FF), jnp.float32)
        return lax.fori_loop(jnp.int32(0), jnp.int32(N_COL), add_column, start_sum).astype(jnp.bfloat16)
    input_grads = lax.map(group_inputs, out_grads)

    def add_group(running, operands):
        acts_group, grad_group = operands
        partial_value = jnp.dot(acts_group.T, grad_group, preferred_element_type=jnp.float32) * keep
        rounded = lax.optimization_barrier(partial_value.astype(jnp.bfloat16))
        return (running + rounded.astype(jnp.float32), None)
    grad, _ = lax.scan(add_group, jnp.zeros((FF, D), jnp.float32), (activations, out_grads))
    new_first = first_decay * first_moment + (1.0 - first_decay) * grad
    new_second = second_decay * second_moment + (1.0 - second_decay) * grad * grad
    step_size = new_first / first_correct / (jnp.sqrt(new_second / second_correct) + adam_epsilon)
    new_weight = keep * (master_weight - learn_rate * step_size)
    return (input_grads, new_weight, new_first, new_second)
```

```python
import jax
import jax.numpy as jnp
from jax import lax
from jax.experimental import pallas as pl
from jax.experimental.pallas import tpu as pltpu
from jax.sharding import Mesh
from jax.sharding import PartitionSpec as P

BLOCK = 128
ROW = ("zh", "core")
COL = ("y", "zl")
ROW_X = ("zh", "core", "x")


first_decay = 0.9
second_decay = 0.999
learn_rate = 0.001
adam_epsilon = 1e-08
first_correct = 1.0 - 0.9**10
second_correct = 1.0 - 0.999**10


def from_everyone(array, axis):
    copies = jnp.broadcast_to(array, (lax.axis_size(axis), *array.shape))
    return lax.all_to_all(copies, axis, split_axis=0, concat_axis=0, tiled=True)


def shifted(array, axis, by):
    peers = lax.axis_size(axis)
    return lax.ppermute(array, axis, [(k, (k + by) % peers) for k in range(peers)])


def expand(block_keep):
    tall, broad = block_keep.shape
    values = block_keep.astype(jnp.float32)
    grown = jnp.broadcast_to(values[:, None, :, None], (tall, BLOCK, broad, BLOCK))
    return grown.reshape(tall * BLOCK, broad * BLOCK)


def run_all(copies):
    for copy in copies:
        copy.start()
    for copy in copies:
        copy.wait()


def ring_place(index, step):
    return lax.rem(index + 4 - step, 4)


def gather_grads(mine, theirs, tile, sems, y):
    cols = mine.shape[-1]
    return [
        pltpu.make_async_copy(
            source.at[:, ring_place(y, s)], tile.at[h, :, :, pl.ds(s * cols, cols)], sems.at[h * 4 + s]
        )
        for h, source in enumerate((mine, theirs))
        for s in range(4)
    ]


def inputs_kernel(place, mine, theirs, w0, w1, w2, w3, out, tile, weights, sems):
    y, core = place[1], place[3]
    cols = w0.shape[-1]
    copies = [
        pltpu.make_async_copy(w, weights.at[:, pl.ds(s * cols, cols)], sems.at[8 + s])
        for s, w in enumerate((w0, w1, w2, w3))
    ]
    run_all(gather_grads(mine, theirs, tile, sems, y) + copies)
    groups, tokens, deep = tile.shape[1:]
    for h in range(2):
        part = lax.dot_general(
            tile[h].reshape(groups * tokens, deep),
            weights[...],
            (((1,), (1,)), ((), ())),
            preferred_element_type=jnp.float32,
        ).astype(jnp.bfloat16)
        where = core if h == 0 else 1 - core
        out[:, where] = part.reshape(groups, *out.shape[2:])


def weights_kernel(place, mine, theirs, a0, a1, a2, a3, o0, o1, o2, o3, tile, acts, sems):
    x, y, zl, core = place[0], place[1], place[2], place[3]
    copies = []
    for t, piece in enumerate((a0, a1, a2, a3)):
        where = ring_place(zl, t)
        half = lax.rem(where // 2 + core, 2)
        for s in range(4):
            copies.append(
                pltpu.make_async_copy(
                    piece.at[s],
                    acts.at[half, ring_place(x, s), lax.rem(where, 2)],
                    sems.at[8 + t * 4 + s],
                )
            )
    run_all(gather_grads(mine, theirs, tile, sems, y) + copies)
    total = tile.shape[0] * tile.shape[1] * tile.shape[2]
    left = acts[...].reshape(total, acts.shape[-1])
    cols = o0.shape[-1]
    for k, out in enumerate((o0, o1, o2, o3)):
        s = (4 - k) % 4
        right = tile[:, :, :, s * cols : (s + 1) * cols].reshape(total, cols)
        out[...] = lax.dot_general(
            left, right, (((0,), (0,)), ((), ())), preferred_element_type=jnp.float32
        ).astype(jnp.bfloat16)


def sum_kernel(parts, out):
    wide = parts.shape[-1]
    for k in range(parts.shape[0]):
        total = parts[k, 0].astype(jnp.float32)
        for j in range(1, parts.shape[1]):
            total = total + parts[k, j].astype(jnp.float32)
        out[:, k * wide : (k + 1) * wide] = total.astype(jnp.bfloat16)


def local_call(kernel, outs, scratch, place, *arrays, flops):
    shapes = [jax.ShapeDtypeStruct(s, jnp.bfloat16) for s in outs]
    single = len(shapes) == 1
    spec = pl.BlockSpec(memory_space=pltpu.VMEM)
    return pl.pallas_call(
        kernel,
        out_shape=shapes[0] if single else shapes,
        in_specs=[pl.BlockSpec(memory_space=pltpu.SMEM)] + [pl.BlockSpec(memory_space=pl.ANY)] * len(arrays),
        out_specs=spec if single else [spec] * len(shapes),
        scratch_shapes=scratch,
        cost_estimate=pl.CostEstimate(flops=flops, bytes_accessed=4 << 20, transcendentals=0),
        compiler_params=pltpu.CompilerParams(vmem_limit_bytes=16 << 20),
    )(place, *arrays)


def body(activations, out_grads, block_mask, master_weight, first_moment, second_moment):
    nx, ny, nl = (lax.axis_size(k) for k in ("x", "y", "zl"))
    x, y, zl, core = (lax.axis_index(k) for k in ("x", "y", "zl", "core"))
    place = jnp.stack([x, y, zl, core]).astype(jnp.int32)
    rows, cols = master_weight.shape
    acts, grads = activations[0], out_grads[0]
    tok, wide = acts.shape
    held = grads.shape[0]

    mask_rows = rows // BLOCK
    keep = expand(lax.dynamic_slice_in_dim(block_mask, x * mask_rows, mask_rows, 0))

    by_zh = from_everyone(grads, "zh")
    own = master_weight.astype(jnp.bfloat16) * keep.astype(jnp.bfloat16)
    weights = [own] + [shifted(own, "y", s) for s in range(1, ny)]

    def cut(s):
        return lax.dynamic_slice_in_dim(acts, (x + s) % nx * rows, rows, 1)

    chunks = [cut(0)] + [shifted(cut(s), "x", s) for s in range(1, nx)]
    by_zh, weights, chunks = lax.optimization_barrier((by_zh, weights, chunks))

    spread = jnp.broadcast_to(by_zh, (nx, *by_zh.shape)).reshape(nx * ny, held, cols)
    mine = lax.all_to_all(spread, ("x", "y"), 0, 0, tiled=True)
    chunk = jnp.stack(chunks)
    pieces = [chunk] + [shifted(chunk, "zl", s) for s in range(1, nl)]
    mine, pieces = lax.optimization_barrier((mine, pieces))
    mine = mine.reshape(nx, ny, held, cols)
    theirs = shifted(mine, "core", 1)

    flops = 2 * nx * 2 * held * ny * cols * rows
    grad_tile = pltpu.VMEM((2, nx, held, ny * cols), jnp.bfloat16)
    part = local_call(
        inputs_kernel,
        [(nx, 2, 2, tok, rows)],
        [grad_tile, pltpu.VMEM((rows, ny * cols), jnp.bfloat16), pltpu.SemaphoreType.DMA((12,))],
        place, mine, theirs, *weights, flops=flops,
    )
    parts = lax.all_to_all(part.reshape(nx * nl, tok, rows), ("x", "zl"), 0, 0, tiled=True)

    got = local_call(
        weights_kernel,
        [(rows, cols)] * ny,
        [grad_tile, pltpu.VMEM((2, nx, 2, tok, rows), jnp.bfloat16), pltpu.SemaphoreType.DMA((24,))],
        place, mine, theirs, *pieces, flops=flops,
    )
    got = [got[0]] + [shifted(got[s], "y", s) for s in range(1, ny)]
    grad = keep * sum(g.astype(jnp.float32) for g in got)

    new_first = first_decay * first_moment + (1.0 - first_decay) * grad
    new_second = second_decay * second_moment + (1.0 - second_decay) * grad * grad
    step_size = new_first / first_correct / (jnp.sqrt(new_second / second_correct) + adam_epsilon)
    new_weight = keep * (master_weight - learn_rate * step_size)

    input_grads = pl.pallas_call(
        sum_kernel, out_shape=jax.ShapeDtypeStruct((tok, wide), jnp.bfloat16)
    )(parts.reshape(nx, nl, tok, rows))
    return (input_grads[None], new_weight, new_first, new_second)


def solution(mesh):
    finer = Mesh(mesh.devices.reshape(4, 2, 4, 4, 4), ("zh", "core", "y", "zl", "x"))
    weight_spec = P(ROW_X, COL)
    in_specs = (P("x", COL, ROW), P("x", ROW, COL), P(ROW, COL), weight_spec, weight_spec, weight_spec)
    out_specs = (P("x", COL, ROW), weight_spec, weight_spec, weight_spec)
    return jax.shard_map(body, mesh=finer, in_specs=in_specs, out_specs=out_specs, check_vma=False)
```

```python
import jax
import jax.numpy as jnp
from jax import lax
from jax.experimental import pallas as pl
from jax.experimental.pallas import tpu as pltpu
from jax.sharding import Mesh
from jax.sharding import PartitionSpec as P

BLOCK = 128
ROW = ("zh", "core")
COL = ("y", "zl")
ROW_X = ("zh", "core", "x")


first_decay = 0.9
second_decay = 0.999
learn_rate = 0.001
adam_epsilon = 1e-08
first_correct = 1.0 - 0.9**10
second_correct = 1.0 - 0.999**10


def from_everyone(array, axis):
    copies = jnp.broadcast_to(array, (lax.axis_size(axis), *array.shape))
    return lax.all_to_all(copies, axis, split_axis=0, concat_axis=0, tiled=True)


def shifted(array, axis, by):
    peers = lax.axis_size(axis)
    return lax.ppermute(array, axis, [(k, (k + by) % peers) for k in range(peers)])


def partners(index):
    first = index + 1 - 2 * (index % 2)
    return (index, first, 3 - index, 3 - first)


def swapped(array, axis, which):
    return lax.ppermute(array, axis, [(k, partners(k)[which]) for k in range(4)])


def expand(block_keep):
    tall, broad = block_keep.shape
    values = block_keep.astype(jnp.float32)
    grown = jnp.broadcast_to(values[:, None, :, None], (tall, BLOCK, broad, BLOCK))
    return grown.reshape(tall * BLOCK, broad * BLOCK)


def ring_place(index, step):
    return lax.rem(index + 4 - step, 4)


def start_all(copies):
    for copy in copies:
        copy.start()
    return copies


def wait_all(copies):
    for copy in copies:
        copy.wait()


def gather_grads(source, tile, sems, y):
    cols = source.shape[-1]
    return [
        pltpu.make_async_copy(source.at[:, place_y], tile.at[:, :, pl.ds(s * cols, cols)], sems.at[s])
        for s, place_y in enumerate(partners(y))
    ]


def half_inputs(where, place, source, near, far, out, tile, weights, result, sems):
    cols = near.shape[-1]
    copies = [
        pltpu.make_async_copy((near, far)[s // 2].at[s % 2], weights.at[:, pl.ds(s * cols, cols)], sems.at[4 + s])
        for s in range(4)
    ]
    wait_all(start_all(gather_grads(source, tile, sems, place[1]) + copies))
    groups, tokens, deep = tile.shape
    step = groups // 2
    sent = []
    for k in range(2):
        mine = pl.ds(k * step, step)
        part = lax.dot_general(
            tile[mine].reshape(step * tokens, deep),
            weights[...],
            (((1,), (1,)), ((), ())),
            preferred_element_type=jnp.float32,
        ).astype(jnp.bfloat16)
        result[mine] = part.reshape(step, *result.shape[1:])
        sent += start_all([pltpu.make_async_copy(result.at[mine], out.at[mine, where], sems.at[8 + k])])
    wait_all(sent)


def own_half_kernel(place, source, near, far, out, *scratch):
    half_inputs(place[3], place, source, near, far, out, *scratch)


def other_half_kernel(place, source, near, far, begun, out, *scratch):
    half_inputs(1 - place[3], place, source, near, far, out, *scratch)


def weights_kernel(place, mine, theirs, a0, a1, a2, a3, o0, o1, o2, o3, tile, acts, turned, sems):
    x, y, zl, core = place[0], place[1], place[2], place[3]
    copies = []
    for t, piece in enumerate((a0, a1, a2, a3)):
        where = ring_place(zl, t)
        half = lax.rem(where // 2 + core, 2)
        for s, place_x in enumerate(partners(x)):
            copies.append(
                pltpu.make_async_copy(
                    piece.at[s],
                    acts.at[half, place_x, lax.rem(where, 2)],
                    sems.at[8 + t * 4 + s],
                )
            )
    start_all(copies)
    tiles = start_all(
        gather_grads(mine, tile.at[0], sems.at[pl.ds(0, 4)], y)
        + gather_grads(theirs, tile.at[1], sems.at[pl.ds(4, 4)], y)
    )
    wait_all(copies)
    total = tile.shape[0] * tile.shape[1] * tile.shape[2]
    turned[...] = acts[...].reshape(total, acts.shape[-1]).T
    wait_all(tiles)
    cols = o0.shape[-1]
    for s, out in enumerate((o0, o1, o2, o3)):
        right = tile[:, :, :, s * cols : (s + 1) * cols].reshape(total, cols)
        out[...] = lax.dot_general(
            turned[...], right, (((1,), (0,)), ((), ())), preferred_element_type=jnp.float32
        ).astype(jnp.bfloat16)


def sum_kernel(parts, out, held, result, sems):
    blocks, peers, _, wide = held.shape
    copies = start_all([pltpu.make_async_copy(parts.at[k], held.at[k], sems.at[k]) for k in range(blocks)])
    sent = []
    for k in range(blocks):
        copies[k].wait()
        total = held[k, 0].astype(jnp.float32)
        for j in range(1, peers):
            total = total + held[k, j].astype(jnp.float32)
        mine = pl.ds(k * wide, wide)
        result[:, mine] = total.astype(jnp.bfloat16)
        sent += start_all([pltpu.make_async_copy(result.at[:, mine], out.at[:, mine], sems.at[blocks + k])])
    wait_all(sent)


def local_call(kernel, outs, scratch, place, *arrays, flops, out_space=pltpu.VMEM, aliases=()):
    shapes = [jax.ShapeDtypeStruct(s, jnp.bfloat16) for s in outs]
    single = len(shapes) == 1
    spec = pl.BlockSpec(memory_space=out_space)
    return pl.pallas_call(
        kernel,
        out_shape=shapes[0] if single else shapes,
        in_specs=[pl.BlockSpec(memory_space=pltpu.SMEM)] + [pl.BlockSpec(memory_space=pl.ANY)] * len(arrays),
        out_specs=spec if single else [spec] * len(shapes),
        scratch_shapes=scratch,
        input_output_aliases=dict(aliases),
        cost_estimate=pl.CostEstimate(flops=flops, bytes_accessed=4 << 20, transcendentals=0),
        compiler_params=pltpu.CompilerParams(vmem_limit_bytes=16 << 20),
    )(place, *arrays)


def body(activations, out_grads, block_mask, master_weight, first_moment, second_moment):
    nx, ny, nl = (lax.axis_size(k) for k in ("x", "y", "zl"))
    x, y, zl, core = (lax.axis_index(k) for k in ("x", "y", "zl", "core"))
    place = jnp.stack([x, y, zl, core]).astype(jnp.int32)
    rows, cols = master_weight.shape
    acts, grads = activations[0], out_grads[0]
    tok, wide = acts.shape
    held = grads.shape[0]

    mask_rows = rows // BLOCK
    keep = expand(lax.dynamic_slice_in_dim(block_mask, x * mask_rows, mask_rows, 0))

    by_zh = from_everyone(grads, "zh")
    own = master_weight.astype(jnp.bfloat16) * keep.astype(jnp.bfloat16)
    near = jnp.stack([own, swapped(own, "y", 1)])
    far = swapped(near, "y", 2)

    def cut(k):
        return lax.dynamic_slice_in_dim(acts, k * rows, rows, 1)

    here, first, second, third = (cut(k) for k in partners(x))
    arrived = swapped(jnp.stack([first, third]), "x", 1)
    crossed = swapped(jnp.stack([second, arrived[1]]), "x", 2)
    chunk = jnp.concatenate([here[None], arrived[:1], crossed])
    by_zh, chunk = lax.optimization_barrier((by_zh, chunk))

    spread = jnp.broadcast_to(by_zh, (nx, *by_zh.shape)).reshape(nx * ny, held, cols)
    mine = lax.all_to_all(spread, ("x", "y"), 0, 0, tiled=True)
    pieces = [chunk] + [shifted(chunk, "zl", s) for s in range(1, nl)]
    mine = mine.reshape(nx, ny, held, cols)
    theirs = shifted(mine, "core", 1)

    flops = 2 * nx * 2 * held * ny * cols * rows
    half_tile = (nx, held, ny * cols)
    scratch = [
        pltpu.VMEM(half_tile, jnp.bfloat16),
        pltpu.VMEM((rows, ny * cols), jnp.bfloat16),
        pltpu.VMEM((nx, 2, tok, rows), jnp.bfloat16),
        pltpu.SemaphoreType.DMA((10,)),
    ]
    shape = [(nx, 2, 2, tok, rows)]
    begun = local_call(own_half_kernel, shape, scratch, place, mine, near, far, flops=flops // 2, out_space=pl.ANY)
    part = local_call(
        other_half_kernel, shape, scratch, place, theirs, near, far, begun,
        flops=flops // 2, out_space=pl.ANY, aliases={4: 0},
    )
    parts = lax.all_to_all(part.reshape(nx * nl, tok, rows), ("x", "zl"), 0, 0, tiled=True)

    got = local_call(
        weights_kernel,
        [(rows, cols)] * ny,
        [
            pltpu.VMEM((2, *half_tile), jnp.bfloat16),
            pltpu.VMEM((2, nx, 2, tok, rows), jnp.bfloat16),
            pltpu.VMEM((rows, nx * 4 * tok), jnp.bfloat16),
            pltpu.SemaphoreType.DMA((24,)),
        ],
        place, mine, theirs, *pieces, flops=flops,
    )
    got = [got[0]] + [swapped(got[s], "y", s) for s in range(1, ny)]
    grad = keep * sum(g.astype(jnp.float32) for g in got)

    new_first = first_decay * first_moment + (1.0 - first_decay) * grad
    new_second = second_decay * second_moment + (1.0 - second_decay) * grad * grad
    step_size = new_first / first_correct / (jnp.sqrt(new_second / second_correct) + adam_epsilon)
    new_weight = keep * (master_weight - learn_rate * step_size)

    input_grads = pl.pallas_call(
        sum_kernel,
        out_shape=jax.ShapeDtypeStruct((tok, wide), jnp.bfloat16),
        in_specs=[pl.BlockSpec(memory_space=pl.ANY)],
        out_specs=pl.BlockSpec(memory_space=pl.ANY),
        scratch_shapes=[
            pltpu.VMEM((nx, nl, tok, rows), jnp.bfloat16),
            pltpu.VMEM((tok, wide), jnp.bfloat16),
            pltpu.SemaphoreType.DMA((2 * nx,)),
        ],
    )(parts.reshape(nx, nl, tok, rows))
    return (input_grads[None], new_weight, new_first, new_second)


def solution(mesh):
    finer = Mesh(mesh.devices.reshape(4, 2, 4, 4, 4), ("zh", "core", "y", "zl", "x"))
    weight_spec = P(ROW_X, COL)
    in_specs = (P("x", COL, ROW), P("x", ROW, COL), P(ROW, COL), weight_spec, weight_spec, weight_spec)
    out_specs = (P("x", COL, ROW), weight_spec, weight_spec, weight_spec)
    return jax.shard_map(body, mesh=finer, in_specs=in_specs, out_specs=out_specs, check_vma=False)
```

```python
import jax
import jax.numpy as jnp
from jax import lax
from jax.experimental import pallas as pl
from jax.experimental.pallas import tpu as pltpu
from jax.sharding import Mesh
from jax.sharding import PartitionSpec as P

BLOCK = 128
ROW = ("zh", "core")
COL = ("y", "zl")
ROW_X = ("zh", "core", "x")


first_decay = 0.9
second_decay = 0.999
learn_rate = 0.001
adam_epsilon = 1e-08
first_correct = 1.0 - 0.9**10
second_correct = 1.0 - 0.999**10


def from_everyone(array, axis):
    copies = jnp.broadcast_to(array, (lax.axis_size(axis), *array.shape))
    return lax.all_to_all(copies, axis, split_axis=0, concat_axis=0, tiled=True)


def shifted(array, axis, by):
    peers = lax.axis_size(axis)
    return lax.ppermute(array, axis, [(k, (k + by) % peers) for k in range(peers)])


def partners(index):
    first = index + 1 - 2 * (index % 2)
    return (index, first, 3 - index, 3 - first)


def swapped(array, axis, which):
    return lax.ppermute(array, axis, [(k, partners(k)[which]) for k in range(4)])


def expand(block_keep):
    tall, broad = block_keep.shape
    values = block_keep.astype(jnp.float32)
    grown = jnp.broadcast_to(values[:, None, :, None], (tall, BLOCK, broad, BLOCK))
    return grown.reshape(tall * BLOCK, broad * BLOCK)


def ring_place(index, step):
    return lax.rem(index + 4 - step, 4)


def start_all(copies):
    for copy in copies:
        copy.start()
    return copies


def wait_all(copies):
    for copy in copies:
        copy.wait()


def gather_grads(source, tile, sems, y):
    cols = source.shape[-1]
    return [
        pltpu.make_async_copy(source.at[place_y], tile.at[:, :, pl.ds(s * cols, cols)], sems.at[s])
        for s, place_y in enumerate(partners(y))
    ]


def half_inputs(where, place, source, near, far, out, tile, weights, result, sems):
    cols = near.shape[-1]
    copies = [
        pltpu.make_async_copy((near, far)[s // 2].at[s % 2], weights.at[:, pl.ds(s * cols, cols)], sems.at[4 + s])
        for s in range(4)
    ]
    wait_all(start_all(gather_grads(source, tile, sems, place[1]) + copies))
    groups, tokens, deep = tile.shape
    step = groups // 2
    sent = []
    for k in range(2):
        mine = pl.ds(k * step, step)
        part = lax.dot_general(
            tile[mine].reshape(step * tokens, deep),
            weights[...],
            (((1,), (1,)), ((), ())),
            preferred_element_type=jnp.float32,
        ).astype(jnp.bfloat16)
        result[mine] = part.reshape(step, *result.shape[1:])
        sent += start_all([pltpu.make_async_copy(result.at[mine], out.at[mine, where], sems.at[8 + k])])
    wait_all(sent)


def own_half_kernel(place, source, near, far, out, *scratch):
    half_inputs(place[3], place, source, near, far, out, *scratch)


def other_half_kernel(place, source, near, far, begun, out, *scratch):
    half_inputs(1 - place[3], place, source, near, far, out, *scratch)


def weights_kernel(place, mine, theirs, a0, a1, a2, a3, o0, o1, o2, o3, tile, acts, turned, sems):
    x, y, zl, core = place[0], place[1], place[2], place[3]
    copies = []
    for t, piece in enumerate((a0, a1, a2, a3)):
        where = ring_place(zl, t)
        half = lax.rem(where // 2 + core, 2)
        for s, place_x in enumerate(partners(x)):
            copies.append(
                pltpu.make_async_copy(
                    piece.at[s],
                    acts.at[half, place_x, lax.rem(where, 2)],
                    sems.at[8 + t * 4 + s],
                )
            )
    start_all(copies)
    tiles = start_all(
        gather_grads(mine, tile.at[0], sems.at[pl.ds(0, 4)], y)
        + gather_grads(theirs, tile.at[1], sems.at[pl.ds(4, 4)], y)
    )
    wait_all(copies)
    total = tile.shape[0] * tile.shape[1] * tile.shape[2]
    turned[...] = acts[...].reshape(total, acts.shape[-1]).T
    wait_all(tiles)
    cols = o0.shape[-1]
    for s, out in enumerate((o0, o1, o2, o3)):
        right = tile[:, :, :, s * cols : (s + 1) * cols].reshape(total, cols)
        out[...] = lax.dot_general(
            turned[...], right, (((1,), (0,)), ((), ())), preferred_element_type=jnp.float32
        ).astype(jnp.bfloat16)


def sum_kernel(parts, out, held, result, sems):
    blocks, peers, _, wide = held.shape
    copies = start_all([pltpu.make_async_copy(parts.at[k], held.at[k], sems.at[k]) for k in range(blocks)])
    sent = []
    for k in range(blocks):
        copies[k].wait()
        total = held[k, 0].astype(jnp.float32)
        for j in range(1, peers):
            total = total + held[k, j].astype(jnp.float32)
        mine = pl.ds(k * wide, wide)
        result[:, mine] = total.astype(jnp.bfloat16)
        sent += start_all([pltpu.make_async_copy(result.at[:, mine], out.at[:, mine], sems.at[blocks + k])])
    wait_all(sent)


def local_call(kernel, outs, scratch, place, *arrays, flops, out_space=pltpu.VMEM, aliases=()):
    shapes = [jax.ShapeDtypeStruct(s, jnp.bfloat16) for s in outs]
    single = len(shapes) == 1
    spec = pl.BlockSpec(memory_space=out_space)
    return pl.pallas_call(
        kernel,
        out_shape=shapes[0] if single else shapes,
        in_specs=[pl.BlockSpec(memory_space=pltpu.SMEM)] + [pl.BlockSpec(memory_space=pl.ANY)] * len(arrays),
        out_specs=spec if single else [spec] * len(shapes),
        scratch_shapes=scratch,
        input_output_aliases=dict(aliases),
        cost_estimate=pl.CostEstimate(flops=flops, bytes_accessed=4 << 20, transcendentals=0),
        compiler_params=pltpu.CompilerParams(vmem_limit_bytes=16 << 20),
    )(place, *arrays)


def body(activations, out_grads, block_mask, master_weight, first_moment, second_moment):
    nx, ny, nl = (lax.axis_size(k) for k in ("x", "y", "zl"))
    x, y, zl, core = (lax.axis_index(k) for k in ("x", "y", "zl", "core"))
    place = jnp.stack([x, y, zl, core]).astype(jnp.int32)
    rows, cols = master_weight.shape
    acts, grads = activations[0], out_grads[0]
    tok, wide = acts.shape
    held = grads.shape[0]

    mask_rows = rows // BLOCK
    keep = expand(lax.dynamic_slice_in_dim(block_mask, x * mask_rows, mask_rows, 0))

    by_zh = from_everyone(grads, "zh")
    own = master_weight.astype(jnp.bfloat16) * keep.astype(jnp.bfloat16)
    near = jnp.stack([own, swapped(own, "y", 1)])
    far = swapped(near, "y", 2)

    def cut(k):
        return lax.dynamic_slice_in_dim(acts, k * rows, rows, 1)

    here, first, second, third = (cut(k) for k in partners(x))
    arrived = swapped(jnp.stack([first, third]), "x", 1)
    crossed = swapped(jnp.stack([second, arrived[1]]), "x", 2)
    chunk = jnp.concatenate([here[None], arrived[:1], crossed])
    by_zh, chunk = lax.optimization_barrier((by_zh, chunk))

    spread = jnp.broadcast_to(by_zh[:, None], (ny, nx, held, cols)).reshape(ny * nx, held, cols)
    mine = lax.all_to_all(spread, ("y", "x"), 0, 0, tiled=True)
    pieces = [chunk] + [shifted(chunk, "zl", s) for s in range(1, nl)]
    mine = mine.reshape(ny, nx, held, cols)
    theirs = shifted(mine, "core", 1)

    flops = 2 * nx * 2 * held * ny * cols * rows
    half_tile = (nx, held, ny * cols)
    scratch = [
        pltpu.VMEM(half_tile, jnp.bfloat16),
        pltpu.VMEM((rows, ny * cols), jnp.bfloat16),
        pltpu.VMEM((nx, 2, tok, rows), jnp.bfloat16),
        pltpu.SemaphoreType.DMA((10,)),
    ]
    shape = [(nx, 2, 2, tok, rows)]
    begun = local_call(own_half_kernel, shape, scratch, place, mine, near, far, flops=flops // 2, out_space=pl.ANY)
    part = local_call(
        other_half_kernel, shape, scratch, place, theirs, near, far, begun,
        flops=flops // 2, out_space=pl.ANY, aliases={4: 0},
    )
    parts = lax.all_to_all(part.reshape(nx * nl, tok, rows), ("x", "zl"), 0, 0, tiled=True)

    got = local_call(
        weights_kernel,
        [(rows, cols)] * ny,
        [
            pltpu.VMEM((2, *half_tile), jnp.bfloat16),
            pltpu.VMEM((2, nx, 2, tok, rows), jnp.bfloat16),
            pltpu.VMEM((rows, nx * 4 * tok), jnp.bfloat16),
            pltpu.SemaphoreType.DMA((24,)),
        ],
        place, mine, theirs, *pieces, flops=flops,
    )
    got = [got[0]] + [swapped(got[s], "y", s) for s in range(1, ny)]
    grad = keep * sum(g.astype(jnp.float32) for g in got)

    new_first = first_decay * first_moment + (1.0 - first_decay) * grad
    new_second = second_decay * second_moment + (1.0 - second_decay) * grad * grad
    step_size = new_first / first_correct / (jnp.sqrt(new_second / second_correct) + adam_epsilon)
    new_weight = keep * (master_weight - learn_rate * step_size)

    input_grads = pl.pallas_call(
        sum_kernel,
        out_shape=jax.ShapeDtypeStruct((tok, wide), jnp.bfloat16),
        in_specs=[pl.BlockSpec(memory_space=pl.ANY)],
        out_specs=pl.BlockSpec(memory_space=pl.ANY),
        scratch_shapes=[
            pltpu.VMEM((nx, nl, tok, rows), jnp.bfloat16),
            pltpu.VMEM((tok, wide), jnp.bfloat16),
            pltpu.SemaphoreType.DMA((2 * nx,)),
        ],
    )(parts.reshape(nx, nl, tok, rows))
    return (input_grads[None], new_weight, new_first, new_second)


def solution(mesh):
    finer = Mesh(mesh.devices.reshape(4, 2, 4, 4, 4), ("zh", "core", "y", "zl", "x"))
    weight_spec = P(ROW_X, COL)
    in_specs = (P("x", COL, ROW), P("x", ROW, COL), P(ROW, COL), weight_spec, weight_spec, weight_spec)
    out_specs = (P("x", COL, ROW), weight_spec, weight_spec, weight_spec)
    return jax.shard_map(body, mesh=finer, in_specs=in_specs, out_specs=out_specs, check_vma=False)
```
